32 devices in a mesh: section: 8 (over y, x, core), tensor: 4 (over z).
Axes of the slice: x: 2, y: 2, z: 4, core: 2. Of those that a mesh axis runs over, the one named last changes fastest.
Arguments:
- key_weight: bfloat16 [8, 8192, 1024], P('section', None, 'tensor'), may hold values from -0.0625 to 0.0625
- value_weight: bfloat16 [8, 8192, 1024], P('section', None, 'tensor'), may hold values from -0.0625 to 0.0625
- norm_gain: bfloat16 [8, 8192], P('section'), may hold values from 0.25 to 1.75
Outputs:
- scaled: bfloat16 [8, 8192, 2048], P(None, ('section', 'tensor'))
- block_scale: float32 [8, 64, 16], P(None, 'section')
The draws below stay inside these ranges and needn't reach their ends.
All inputs are finite; a program needn't handle non-finite values.
Results may differ from the reference program's by a relative error of at most 0.0056.
Values may be sent and summed in bfloat16 or wider, within the bound.
No kernel may reach another device: no remote copies, remote signals or barrier semaphores. Data moves between devices by JAX's collectives and lax.ppermute only.
A program may use at most 128 MiB of HBM per device.

```python
import jax
import jax.numpy as jnp
from jax import lax

D = 8192
BLOCK = 128
LAYERS = 8
KVW = 1024


def levels(own_key, extent, cuts, smallest, top_value):
    factor_of, own = 1.0, jax.random.fold_in(own_key, 6)
    for position, parts in cuts:
        draws = jnp.exp(jax.random.uniform(jax.random.fold_in(own, position), (parts,), jnp.float32, smallest / len(cuts), top_value / len(cuts)))
        factor_of = factor_of * jnp.repeat(draws, extent[position] // parts).reshape([-1 if axis == position else 1 for axis in range(len(extent))])
    return factor_of


def gaussian(own_key, extent, scale, reach, shards=(), held_as=jnp.bfloat16):
    result = jax.random.normal(own_key, extent, jnp.float32) * scale
    if len(shards) > 0:
        result = levels(own_key, extent, shards, -0.22, 0.18) * result
    return jnp.clip(result, min=-reach, max=reach).astype(held_as)


def setup_inputs(seed: int = 0) -> dict:
    splits = jax.random.split(jax.random.key(seed), 4)
    return {
        "key_weight": gaussian(splits[0], (LAYERS, D, KVW), D ** -0.5, 0.0625, ((0, 8), (2, 4))),
        "value_weight": gaussian(splits[1], (LAYERS, D, KVW), D ** -0.5, 0.0625, ((0, 8), (2, 4))),
        "norm_gain": jnp.clip(1.0 + 0.15 * jax.random.normal(splits[2], (LAYERS, D), jnp.float32), 0.25, 1.75).astype(jnp.bfloat16),
    }


scale_floor = 0.00390625


def quantize_layer(inputs):
    key_layer, value_layer, gain_layer = inputs
    stacked = jnp.concatenate([key_layer, value_layer], axis=1)
    folded = (gain_layer.astype(jnp.float32)[:, None] * stacked.astype(jnp.float32)).astype(jnp.bfloat16)
    folded = lax.optimization_barrier(folded).astype(jnp.float32)
    blocks = folded.reshape(D // BLOCK, BLOCK, 2 * KVW // BLOCK, BLOCK)
    block_max = jnp.max(jnp.abs(blocks), axis=(1, 3))
    block_scale = jnp.maximum(block_max, scale_floor)
    scaled = (blocks / block_scale[:, None, :, None]).astype(jnp.bfloat16).reshape(D, 2 * KVW)
    return scaled, block_scale


def reference(key_weight, value_weight, norm_gain):
    scaled, block_scale = lax.map(quantize_layer, (key_weight, value_weight, norm_gain))
    return scaled, block_scale
```

```python
import functools

import jax
import jax.numpy as jnp
from jax import lax
from jax.experimental import pallas as pl
from jax.experimental.pallas import tpu as pltpu
from jax.sharding import PartitionSpec as P

BLOCK = 128
AXES = ("section", "tensor")

scale_floor = 0.00390625


def partner(index, step, count):
    if count & (count - 1) == 0:
        return index ^ step
    return (index + step) % count


def origin(index, step, count):
    if count & (count - 1) == 0:
        return index ^ step
    return (index + count - step) % count


def column_gain(gain):
    return jnp.broadcast_to(gain, (BLOCK, BLOCK)).T


def fold(weight, gain):
    return (weight.astype(jnp.float32) * gain).astype(jnp.bfloat16).astype(jnp.float32)


def block_max(folded):
    largest = jnp.max(jnp.max(jnp.abs(folded), axis=0, keepdims=True), axis=1, keepdims=True)
    return jnp.maximum(largest, scale_floor)


def pack_kernel(
    steps, sections_count, ranks_count, shares, key_ref, value_ref, gain_ref, out_ref, raw, gain, sems
):
    section = lax.axis_index("section")
    rank = lax.axis_index("tensor")
    rows, head_cols = raw.shape[1:]
    to_section = partner(section, steps[0], sections_count)
    to_unit = partner(rank // shares, steps[1], ranks_count // shares)
    first = pl.multiple_of((to_section * (ranks_count // shares) + to_unit) * rows, rows)
    copies = [
        pltpu.make_async_copy(key_ref.at[0, pl.ds(first, rows)], raw.at[0], sems.at[0]),
        pltpu.make_async_copy(value_ref.at[0, pl.ds(first, rows)], raw.at[1], sems.at[1]),
        pltpu.make_async_copy(gain_ref.at[:, pl.ds(first, rows)], gain, sems.at[2]),
    ]
    for copy in copies:
        copy.start()
    for copy in reversed(copies):
        copy.wait()
    share_rows = rows // shares
    for row in range(0, rows, BLOCK):
        gains = column_gain(gain[:, row : row + BLOCK].astype(jnp.float32))
        for kind in range(2):
            for col in range(0, head_cols, BLOCK):
                folded = fold(raw[kind, row : row + BLOCK, col : col + BLOCK], gains)
                scaled = (folded / block_max(folded)).astype(jnp.bfloat16)
                to = kind * head_cols + col
                if shares == 1:
                    out_ref[0, row : row + BLOCK, to : to + BLOCK] = scaled
                    continue
                for part in range(BLOCK // share_rows):
                    place = origin(row // share_rows + part, rank % shares, shares)
                    out_ref[place, :, to : to + BLOCK] = scaled[
                        part * share_rows : (part + 1) * share_rows
                    ]


def pack(steps, sections_count, ranks_count, key_weight, value_weight, norm_gain):
    model_rows, head_cols = key_weight.shape[1:]
    row_share = model_rows // (sections_count * ranks_count)
    shares = max(1, BLOCK // row_share)
    rows = row_share * shares
    any_ref = pl.BlockSpec(memory_space=pl.ANY)
    return pl.pallas_call(
        functools.partial(pack_kernel, steps, sections_count, ranks_count, shares),
        out_shape=jax.ShapeDtypeStruct((shares, row_share, 2 * head_cols), jnp.bfloat16),
        in_specs=[any_ref] * 3,
        out_specs=pl.BlockSpec(memory_space=pltpu.VMEM),
        scratch_shapes=[
            pltpu.VMEM((2, rows, head_cols), jnp.bfloat16),
            pltpu.VMEM((1, rows), jnp.bfloat16),
            pltpu.SemaphoreType.DMA((3,)),
        ],
        compiler_params=pltpu.CompilerParams(vmem_limit_bytes=4 * 2**20),
        cost_estimate=pl.CostEstimate(
            flops=rows * head_cols * 40, bytes_accessed=rows * head_cols * 8, transcendentals=0
        ),
        name="pack",
    )(key_weight, value_weight, norm_gain)


def place_kernel(steps, sections_count, ranks_count, has_out, *refs):
    blocks = refs[: len(steps)]
    out_ref, sems = refs[len(steps) + has_out :]
    section = lax.axis_index("section")
    rank = lax.axis_index("tensor")
    head_cols = blocks[0].shape[1] // 2
    copies = []
    for index, (far, near) in enumerate(steps):
        layer = origin(section, far, sections_count)
        head = origin(rank, near, ranks_count)
        for kind in range(2):
            first = pl.multiple_of((kind * ranks_count + head) * head_cols, head_cols)
            copies.append(
                pltpu.make_async_copy(
                    blocks[index].at[:, pl.ds(kind * head_cols, head_cols)],
                    out_ref.at[layer, :, pl.ds(first, head_cols)],
                    sems.at[2 * index + kind],
                )
            )
    for copy in copies:
        copy.start()
    for copy in copies:
        copy.wait()


def place(steps, sections_count, ranks_count, blocks, out):
    rows, cols = blocks[0].shape
    shape = jax.ShapeDtypeStruct((sections_count, rows, ranks_count * cols), jnp.bfloat16)
    has_out = 0 if out is None else 1
    any_ref = pl.BlockSpec(memory_space=pl.ANY)
    return pl.pallas_call(
        functools.partial(place_kernel, steps, sections_count, ranks_count, has_out),
        out_shape=shape,
        in_specs=[pl.BlockSpec(memory_space=pltpu.VMEM)] * len(blocks) + [any_ref] * has_out,
        out_specs=any_ref,
        scratch_shapes=[pltpu.SemaphoreType.DMA((2 * len(steps),))],
        input_output_aliases={len(blocks): 0} if has_out else {},
        compiler_params=pltpu.CompilerParams(vmem_limit_bytes=4 * 2**20),
        cost_estimate=pl.CostEstimate(
            flops=len(steps) * rows * cols, bytes_accessed=len(steps) * rows * cols * 4, transcendentals=0
        ),
        name="place",
    )(*blocks, *([] if out is None else [out]))


def scales_kernel(key_ref, value_ref, gain_ref, out_ref):
    rows, head_cols = key_ref.shape[1:]
    ranks_count = out_ref.shape[1]
    rank = lax.axis_index("tensor")
    cols_here = head_cols // BLOCK
    shape = (rows // BLOCK, BLOCK)
    row_of = lax.broadcasted_iota(jnp.int32, shape, 0)
    lane_of = lax.broadcasted_iota(jnp.int32, shape, 1)
    found = jnp.zeros(shape, jnp.float32)
    for row in range(rows // BLOCK):
        span = slice(row * BLOCK, (row + 1) * BLOCK)
        gains = column_gain(gain_ref[:, span].astype(jnp.float32))
        for kind, ref in enumerate((key_ref, value_ref)):
            for col in range(cols_here):
                folded = fold(ref[0, span, col * BLOCK : (col + 1) * BLOCK], gains)
                lane = (kind * ranks_count + rank) * cols_here + col
                here = jnp.logical_and(row_of == row, lane_of == lane)
                found = jnp.where(here, block_max(folded), found)
    for copy in range(ranks_count):
        out_ref[0, copy] = found.astype(jnp.bfloat16)


def scales(sections_count, ranks_count, key_weight, value_weight, norm_gain):
    model_rows, head_cols = key_weight.shape[1:]
    rows = model_rows // sections_count
    weight_spec = pl.BlockSpec((1, rows, head_cols), lambda i: (0, i, 0))
    return pl.pallas_call(
        scales_kernel,
        grid=(sections_count,),
        out_shape=jax.ShapeDtypeStruct(
            (sections_count, ranks_count, rows // BLOCK, BLOCK), jnp.bfloat16
        ),
        in_specs=[weight_spec, weight_spec, pl.BlockSpec((1, rows), lambda i: (0, i))],
        out_specs=pl.BlockSpec((1, ranks_count, rows // BLOCK, BLOCK), lambda i: (i, 0, 0, 0)),
        compiler_params=pltpu.CompilerParams(vmem_limit_bytes=8 * 2**20),
        cost_estimate=pl.CostEstimate(
            flops=model_rows * head_cols * 20, bytes_accessed=model_rows * head_cols * 4, transcendentals=0
        ),
        name="scales",
    )(key_weight, value_weight, norm_gain)


def on_device(key_weight, value_weight, norm_gain):
    sections_count = lax.axis_size("section")
    ranks_count = lax.axis_size("tensor")
    sizes = (sections_count, ranks_count)
    model_rows, head_cols = key_weight.shape[1:]
    row_share = model_rows // (sections_count * ranks_count)
    shares = max(1, BLOCK // row_share)
    arrived = {}
    for far in range(sections_count):
        for unit in reversed(range(ranks_count // shares)):
            packed = pack((far, unit), *sizes, key_weight, value_weight, norm_gain)
            for part in range(shares):
                near = unit * shares + part
                pairs = [
                    (
                        section * ranks_count + rank,
                        partner(section, far, sections_count) * ranks_count
                        + partner(rank, near, ranks_count),
                    )
                    for section in range(sections_count)
                    for rank in range(ranks_count)
                ]
                block = packed[part]
                if (far, near) != (0, 0):
                    with jax.named_scope(f"send_{far}_{near}"):
                        block = lax.ppermute(block, AXES, pairs)
                arrived[far, near] = block
    sent = scales(*sizes, key_weight, value_weight, norm_gain)
    got = lax.all_to_all(
        sent.reshape((sections_count * ranks_count,) + sent.shape[2:]), AXES, 0, 0, tiled=True
    )
    col_blocks = 2 * ranks_count * head_cols // BLOCK
    block_scale = jnp.max(got.reshape(sent.shape), axis=1)[:, :, :col_blocks].astype(jnp.float32)
    out = None
    for far in range(sections_count):
        steps = [(far, near) for near in range(ranks_count)]
        out = place(steps, *sizes, [arrived[step] for step in steps], out)
    return (out, block_scale)


def solution(mesh):
    placed = (P("section", None, "tensor"), P("section", None, "tensor"), P("section", None))
    return jax.shard_map(
        on_device,
        mesh=mesh,
        in_specs=placed,
        out_specs=(P(None, AXES, None), P(None, "section", None)),
        check_vma=False,
    )
```

```python
import functools

import jax
import jax.numpy as jnp
from jax import lax
from jax.experimental import pallas as pl
from jax.experimental.pallas import tpu as pltpu
from jax.sharding import PartitionSpec as P


BLOCK = 128
AXES = ("section", "tensor")

scale_floor = 0.00390625


def partner(index, step, count):
    if count & (count - 1) == 0:
        return index ^ step
    return (index + step) % count


def origin(index, step, count):
    if count & (count - 1) == 0:
        return index ^ step
    return (index + count - step) % count


def column_gain(gain):
    return jnp.broadcast_to(gain, (BLOCK, BLOCK)).T


def fold(weight, gain):
    return (weight.astype(jnp.float32) * gain).astype(jnp.bfloat16).astype(jnp.float32)


def block_max(folded):
    largest = jnp.max(jnp.max(jnp.abs(folded), axis=0, keepdims=True), axis=1, keepdims=True)
    return jnp.maximum(largest, scale_floor)


def pack_kernel(
    steps, sections_count, ranks_count, shares, key_ref, value_ref, gain_ref, out_ref, raw, gain, sems
):
    section = lax.axis_index("section")
    rank = lax.axis_index("tensor")
    rows, head_cols = raw.shape[1:]
    to_section = partner(section, steps[0], sections_count)
    to_unit = partner(rank // shares, steps[1], ranks_count // shares)
    first = pl.multiple_of((to_section * (ranks_count // shares) + to_unit) * rows, rows)
    copies = [
        pltpu.make_async_copy(key_ref.at[0, pl.ds(first, rows)], raw.at[0], sems.at[0]),
        pltpu.make_async_copy(value_ref.at[0, pl.ds(first, rows)], raw.at[1], sems.at[1]),
        pltpu.make_async_copy(gain_ref.at[:, pl.ds(first, rows)], gain, sems.at[2]),
    ]
    for copy in copies:
        copy.start()
    for copy in reversed(copies):
        copy.wait()
    share_rows = rows // shares
    for row in range(0, rows, BLOCK):
        gains = column_gain(gain[:, row : row + BLOCK].astype(jnp.float32))
        for kind in range(2):
            for col in range(0, head_cols, BLOCK):
                folded = fold(raw[kind, row : row + BLOCK, col : col + BLOCK], gains)
                scaled = (folded / block_max(folded)).astype(jnp.bfloat16)
                to = kind * head_cols + col
                if shares == 1:
                    out_ref[0, row : row + BLOCK, to : to + BLOCK] = scaled
                    continue
                for part in range(BLOCK // share_rows):
                    place = origin(row // share_rows + part, rank % shares, shares)
                    out_ref[place, :, to : to + BLOCK] = scaled[
                        part * share_rows : (part + 1) * share_rows
                    ]


def pack(steps, sections_count, ranks_count, weights):
    key_weight, value_weight, norm_gain = weights
    model_rows, head_cols = key_weight.shape[1:]
    row_share = model_rows // (sections_count * ranks_count)
    shares = max(1, BLOCK // row_share)
    rows = row_share * shares
    any_ref = pl.BlockSpec(memory_space=pl.ANY)
    return pl.pallas_call(
        functools.partial(pack_kernel, steps, sections_count, ranks_count, shares),
        out_shape=jax.ShapeDtypeStruct((shares, row_share, 2 * head_cols), jnp.bfloat16),
        in_specs=[any_ref] * 3,
        out_specs=pl.BlockSpec(memory_space=pltpu.VMEM),
        scratch_shapes=[
            pltpu.VMEM((2, rows, head_cols), jnp.bfloat16),
            pltpu.VMEM((1, rows), jnp.bfloat16),
            pltpu.SemaphoreType.DMA((3,)),
        ],
        compiler_params=pltpu.CompilerParams(vmem_limit_bytes=60 * 2**20),
        cost_estimate=pl.CostEstimate(
            flops=rows * head_cols * 40, bytes_accessed=rows * head_cols * 8, transcendentals=0
        ),
        name="pack",
    )(key_weight, value_weight, norm_gain)


def place_kernel(steps, sections_count, ranks_count, has_out, *refs):
    blocks = refs[: len(steps)]
    out_ref, sems = refs[len(steps) + has_out :]
    section = lax.axis_index("section")
    rank = lax.axis_index("tensor")
    head_cols = blocks[0].shape[1] // 2
    copies = []
    for index, (far, near) in enumerate(steps):
        layer = origin(section, far, sections_count)
        head = origin(rank, near, ranks_count)
        for kind in range(2):
            first = pl.multiple_of((kind * ranks_count + head) * head_cols, head_cols)
            copies.append(
                pltpu.make_async_copy(
                    blocks[index].at[:, pl.ds(kind * head_cols, head_cols)],
                    out_ref.at[layer, :, pl.ds(first, head_cols)],
                    sems.at[2 * index + kind],
                )
            )
    for copy in copies:
        copy.start()
    for copy in copies:
        copy.wait()


def place(steps, sections_count, ranks_count, blocks, out):
    rows, cols = blocks[0].shape
    shape = jax.ShapeDtypeStruct((sections_count, rows, ranks_count * cols), jnp.bfloat16)
    has_out = 0 if out is None else 1
    any_ref = pl.BlockSpec(memory_space=pl.ANY)
    return pl.pallas_call(
        functools.partial(place_kernel, steps, sections_count, ranks_count, has_out),
        out_shape=shape,
        in_specs=[pl.BlockSpec(memory_space=pltpu.VMEM)] * len(blocks) + [any_ref] * has_out,
        out_specs=any_ref,
        scratch_shapes=[pltpu.SemaphoreType.DMA((2 * len(steps),))],
        input_output_aliases={len(blocks): 0} if has_out else {},
        compiler_params=pltpu.CompilerParams(vmem_limit_bytes=4 * 2**20),
        cost_estimate=pl.CostEstimate(
            flops=len(steps) * rows * cols, bytes_accessed=len(steps) * rows * cols * 4, transcendentals=0
        ),
        name="place",
    )(*blocks, *([] if out is None else [out]))


def scales_kernel(key_ref, value_ref, gain_ref, out_ref):
    rows, head_cols = key_ref.shape[1:]
    ranks_count = out_ref.shape[1]
    rank = lax.axis_index("tensor")
    cols_here = head_cols // BLOCK
    shape = (rows // BLOCK, BLOCK)
    row_of = lax.broadcasted_iota(jnp.int32, shape, 0)
    lane_of = lax.broadcasted_iota(jnp.int32, shape, 1)
    found = jnp.zeros(shape, jnp.float32)
    for row in range(rows // BLOCK):
        span = slice(row * BLOCK, (row + 1) * BLOCK)
        gains = column_gain(gain_ref[:, span].astype(jnp.float32))
        for kind, ref in enumerate((key_ref, value_ref)):
            for col in range(cols_here):
                folded = fold(ref[0, span, col * BLOCK : (col + 1) * BLOCK], gains)
                lane = (kind * ranks_count + rank) * cols_here + col
                here = jnp.logical_and(row_of == row, lane_of == lane)
                found = jnp.where(here, block_max(folded), found)
    for copy in range(ranks_count):
        out_ref[0, copy] = found.astype(jnp.bfloat16)


def scales(sections_count, ranks_count, weights):
    key_weight, value_weight, norm_gain = weights
    model_rows, head_cols = key_weight.shape[1:]
    rows = model_rows // sections_count
    weight_spec = pl.BlockSpec((1, rows, head_cols), lambda i: (0, i, 0))
    return pl.pallas_call(
        scales_kernel,
        grid=(sections_count,),
        out_shape=jax.ShapeDtypeStruct(
            (sections_count, ranks_count, rows // BLOCK, BLOCK), jnp.bfloat16
        ),
        in_specs=[weight_spec, weight_spec, pl.BlockSpec((1, rows), lambda i: (0, i))],
        out_specs=pl.BlockSpec((1, ranks_count, rows // BLOCK, BLOCK), lambda i: (i, 0, 0, 0)),
        compiler_params=pltpu.CompilerParams(vmem_limit_bytes=60 * 2**20),
        cost_estimate=pl.CostEstimate(
            flops=model_rows * head_cols * 20, bytes_accessed=model_rows * head_cols * 4, transcendentals=0
        ),
        name="scales",
    )(key_weight, value_weight, norm_gain)


def send_order(sections_count, units_count):
    half = units_count // 2
    far_steps = [(far, unit) for far in range(sections_count) for unit in reversed(range(half, units_count))]
    near_steps = [(far, unit) for far in range(sections_count) for unit in reversed(range(half))]
    near_steps = near_steps[half:] + near_steps[:half]
    order = far_steps[:2]
    for index, step in enumerate(far_steps[2:]):
        order += near_steps[index : index + 1] + [step]
    rest = near_steps[len(far_steps) - 2 :]
    return order[:2] + rest[:-1] + order[2:] + rest[-1:]


def on_device(key_weight, value_weight, norm_gain):
    sections_count = lax.axis_size("section")
    ranks_count = lax.axis_size("tensor")
    sizes = (sections_count, ranks_count)
    weights = (key_weight, value_weight, norm_gain)
    model_rows, head_cols = key_weight.shape[1:]
    row_share = model_rows // (sections_count * ranks_count)
    shares = max(1, BLOCK // row_share)
    order = send_order(sections_count, ranks_count // shares)
    arrived = {}
    for far, unit in order:
        packed = pack((far, unit), *sizes, weights)
        for part in range(shares):
            near = unit * shares + part
            pairs = [
                (
                    section * ranks_count + rank,
                    partner(section, far, sections_count) * ranks_count
                    + partner(rank, near, ranks_count),
                )
                for section in range(sections_count)
                for rank in range(ranks_count)
            ]
            block = packed[part]
            if (far, near) != (0, 0):
                block = lax.ppermute(block, AXES, pairs)
            arrived[far, near] = block
    sent_scales = scales(*sizes, weights)
    got = lax.all_to_all(
        sent_scales.reshape((sections_count * ranks_count,) + sent_scales.shape[2:]), AXES, 0, 0, tiled=True
    )
    col_blocks = 2 * ranks_count * head_cols // BLOCK
    block_scale = jnp.max(got.reshape(sent_scales.shape), axis=1)[:, :, :col_blocks].astype(jnp.float32)
    last = tuple(unit * shares + shares - 1 if i else unit for i, unit in enumerate(order[-2]))
    out = None
    groups = [[(far, near) for near in range(ranks_count) if (far, near) != last] for far in range(sections_count)]
    for steps in groups + [[last]]:
        out = place(steps, *sizes, [arrived[step] for step in steps], out)
    return (out, block_scale)


def solution(mesh):
    placed = (P("section", None, "tensor"), P("section", None, "tensor"), P("section", None))

    return jax.shard_map(
        on_device,
        mesh=mesh,
        in_specs=placed,
        out_specs=(P(None, AXES, None), P(None, "section", None)),
        check_vma=False,
    )
```

```python
import functools

import jax
import jax.numpy as jnp
from jax import lax
from jax.experimental import pallas as pl
from jax.experimental.pallas import tpu as pltpu
from jax.sharding import PartitionSpec as P


BLOCK = 128
AXES = ("section", "tensor")

scale_floor = 0.00390625


def partner(index, step, count):
    if count & (count - 1) == 0:
        return index ^ step
    return (index + step) % count


def origin(index, step, count):
    if count & (count - 1) == 0:
        return index ^ step
    return (index + count - step) % count


def column_gain(gain):
    return jnp.broadcast_to(gain, (BLOCK, BLOCK)).T


def fold(weight, gain):
    return (weight.astype(jnp.float32) * gain).astype(jnp.bfloat16).astype(jnp.float32)


def block_max(folded):
    largest = jnp.max(jnp.max(jnp.abs(folded), axis=0, keepdims=True), axis=1, keepdims=True)
    return jnp.maximum(largest, scale_floor)


def pack_kernel(
    steps, sections_count, ranks_count, shares, key_ref, value_ref, gain_ref, out_ref, raw, gain, sems
):
    section = lax.axis_index("section")
    rank = lax.axis_index("tensor")
    rows, head_cols = raw.shape[1:]
    to_section = partner(section, steps[0], sections_count)
    to_unit = partner(rank // shares, steps[1], ranks_count // shares)
    first = pl.multiple_of((to_section * (ranks_count // shares) + to_unit) * rows, rows)
    copies = [
        pltpu.make_async_copy(key_ref.at[0, pl.ds(first, rows)], raw.at[0], sems.at[0]),
        pltpu.make_async_copy(value_ref.at[0, pl.ds(first, rows)], raw.at[1], sems.at[1]),
        pltpu.make_async_copy(gain_ref.at[:, pl.ds(first, rows)], gain, sems.at[2]),
    ]
    for copy in copies:
        copy.start()
    for copy in reversed(copies):
        copy.wait()
    share_rows = rows // shares
    for row in range(0, rows, BLOCK):
        gains = column_gain(gain[:, row : row + BLOCK].astype(jnp.float32))
        for kind in range(2):
            for col in range(0, head_cols, BLOCK):
                folded = fold(raw[kind, row : row + BLOCK, col : col + BLOCK], gains)
                scaled = (folded / block_max(folded)).astype(jnp.bfloat16)
                to = kind * head_cols + col
                if shares == 1:
                    out_ref[0, row : row + BLOCK, to : to + BLOCK] = scaled
                    continue
                for part in range(BLOCK // share_rows):
                    place = origin(row // share_rows + part, rank % shares, shares)
                    out_ref[place, :, to : to + BLOCK] = scaled[
                        part * share_rows : (part + 1) * share_rows
                    ]


def pack(steps, sections_count, ranks_count, weights):
    key_weight, value_weight, norm_gain = weights
    model_rows, head_cols = key_weight.shape[1:]
    row_share = model_rows // (sections_count * ranks_count)
    shares = max(1, BLOCK // row_share)
    rows = row_share * shares
    any_ref = pl.BlockSpec(memory_space=pl.ANY)
    return pl.pallas_call(
        functools.partial(pack_kernel, steps, sections_count, ranks_count, shares),
        out_shape=jax.ShapeDtypeStruct((shares, row_share, 2 * head_cols), jnp.bfloat16),
        in_specs=[any_ref] * 3,
        out_specs=pl.BlockSpec(memory_space=pltpu.VMEM),
        scratch_shapes=[
            pltpu.VMEM((2, rows, head_cols), jnp.bfloat16),
            pltpu.VMEM((1, rows), jnp.bfloat16),
            pltpu.SemaphoreType.DMA((3,)),
        ],
        compiler_params=pltpu.CompilerParams(vmem_limit_bytes=60 * 2**20),
        cost_estimate=pl.CostEstimate(
            flops=rows * head_cols * 40, bytes_accessed=rows * head_cols * 8, transcendentals=0
        ),
        name="pack",
    )(key_weight, value_weight, norm_gain)


def place_kernel(steps, sections_count, ranks_count, has_out, *refs):
    blocks = refs[: len(steps)]
    out_ref, sems = refs[len(steps) + has_out :]
    section = lax.axis_index("section")
    rank = lax.axis_index("tensor")
    head_cols = blocks[0].shape[1] // 2
    copies = []
    for index, (far, near) in enumerate(steps):
        layer = origin(section, far, sections_count)
        head = origin(rank, near, ranks_count)
        for kind in range(2):
            first = pl.multiple_of((kind * ranks_count + head) * head_cols, head_cols)
            copies.append(
                pltpu.make_async_copy(
                    blocks[index].at[:, pl.ds(kind * head_cols, head_cols)],
                    out_ref.at[layer, :, pl.ds(first, head_cols)],
                    sems.at[2 * index + kind],
                )
            )
    for copy in copies:
        copy.start()
    for copy in copies:
        copy.wait()


def place(steps, sections_count, ranks_count, blocks, out):
    rows, cols = blocks[0].shape
    shape = jax.ShapeDtypeStruct((sections_count, rows, ranks_count * cols), jnp.bfloat16)
    has_out = 0 if out is None else 1
    any_ref = pl.BlockSpec(memory_space=pl.ANY)
    return pl.pallas_call(
        functools.partial(place_kernel, steps, sections_count, ranks_count, has_out),
        out_shape=shape,
        in_specs=[pl.BlockSpec(memory_space=pltpu.VMEM)] * len(blocks) + [any_ref] * has_out,
        out_specs=any_ref,
        scratch_shapes=[pltpu.SemaphoreType.DMA((2 * len(steps),))],
        input_output_aliases={len(blocks): 0} if has_out else {},
        compiler_params=pltpu.CompilerParams(vmem_limit_bytes=4 * 2**20),
        cost_estimate=pl.CostEstimate(
            flops=len(steps) * rows * cols, bytes_accessed=len(steps) * rows * cols * 4, transcendentals=0
        ),
        name="place",
    )(*blocks, *([] if out is None else [out]))


def scales_kernel(key_ref, value_ref, gain_ref, out_ref):
    rows, head_cols = key_ref.shape[1:]
    ranks_count = out_ref.shape[1]
    rank = lax.axis_index("tensor")
    cols_here = head_cols // BLOCK
    shape = (rows // BLOCK, BLOCK)
    row_of = lax.broadcasted_iota(jnp.int32, shape, 0)
    lane_of = lax.broadcasted_iota(jnp.int32, shape, 1)
    found = jnp.zeros(shape, jnp.float32)
    for row in range(rows // BLOCK):
        span = slice(row * BLOCK, (row + 1) * BLOCK)
        gains = column_gain(gain_ref[:, span].astype(jnp.float32))
        for kind, ref in enumerate((key_ref, value_ref)):
            for col in range(cols_here):
                folded = fold(ref[0, span, col * BLOCK : (col + 1) * BLOCK], gains)
                lane = (kind * ranks_count + rank) * cols_here + col
                here = jnp.logical_and(row_of == row, lane_of == lane)
                found = jnp.where(here, block_max(folded), found)
    for copy in range(ranks_count):
        out_ref[0, copy] = found.astype(jnp.bfloat16)


def scales(sections_count, ranks_count, weights):
    key_weight, value_weight, norm_gain = weights
    model_rows, head_cols = key_weight.shape[1:]
    rows = model_rows // sections_count
    weight_spec = pl.BlockSpec((1, rows, head_cols), lambda i: (0, i, 0))
    return pl.pallas_call(
        scales_kernel,
        grid=(sections_count,),
        out_shape=jax.ShapeDtypeStruct(
            (sections_count, ranks_count, rows // BLOCK, BLOCK), jnp.bfloat16
        ),
        in_specs=[weight_spec, weight_spec, pl.BlockSpec((1, rows), lambda i: (0, i))],
        out_specs=pl.BlockSpec((1, ranks_count, rows // BLOCK, BLOCK), lambda i: (i, 0, 0, 0)),
        compiler_params=pltpu.CompilerParams(vmem_limit_bytes=60 * 2**20),
        cost_estimate=pl.CostEstimate(
            flops=model_rows * head_cols * 20, bytes_accessed=model_rows * head_cols * 4, transcendentals=0
        ),
        name="scales",
    )(key_weight, value_weight, norm_gain)


def send_order(sections_count, units_count):
    sections = list(range(sections_count))
    if sections_count % 4 == 0:
        sections = [x for step in range(sections_count // 2) for x in (step, step ^ 3 * sections_count // 4)]
    half = units_count // 2
    crossing = [(far, unit) for far in sections for unit in reversed(range(half, units_count))]
    others = [(far, unit) for far in sections for unit in reversed(range(half))]
    others.remove((0, 0))
    order = crossing[:2]
    placed = 0
    for index, step in enumerate(crossing[2:], 1):
        until = -(-len(others) * index // (len(crossing) - 2))
        order += others[placed:until] + [step]
        placed = until
    return order + [(0, 0)]


def on_device(key_weight, value_weight, norm_gain):
    sections_count = lax.axis_size("section")
    ranks_count = lax.axis_size("tensor")
    sizes = (sections_count, ranks_count)
    weights = (key_weight, value_weight, norm_gain)
    model_rows, head_cols = key_weight.shape[1:]
    row_share = model_rows // (sections_count * ranks_count)
    shares = max(1, BLOCK // row_share)
    order = send_order(sections_count, ranks_count // shares)
    arrived = {}
    for far, unit in order:
        packed = pack((far, unit), *sizes, weights)
        for part in range(shares):
            near = unit * shares + part
            pairs = [
                (
                    section * ranks_count + rank,
                    partner(section, far, sections_count) * ranks_count
                    + partner(rank, near, ranks_count),
                )
                for section in range(sections_count)
                for rank in range(ranks_count)
            ]
            block = packed[part]
            if (far, near) != (0, 0):
                block = lax.ppermute(block, AXES, pairs)
            arrived[far, near] = block
    sent_scales = scales(*sizes, weights)
    got = lax.all_to_all(
        sent_scales.reshape((sections_count * ranks_count,) + sent_scales.shape[2:]), AXES, 0, 0, tiled=True
    )
    col_blocks = 2 * ranks_count * head_cols // BLOCK
    block_scale = jnp.max(got.reshape(sent_scales.shape), axis=1)[:, :, :col_blocks].astype(jnp.float32)
    last = tuple(unit * shares + shares - 1 if i else unit for i, unit in enumerate(order[-2]))
    out = None
    groups = [[(far, near) for near in range(ranks_count) if (far, near) != last] for far in range(sections_count)]
    for steps in groups + [[last]]:
        out = place(steps, *sizes, [arrived[step] for step in steps], out)
    return (out, block_scale)


def solution(mesh):
    placed = (P("section", None, "tensor"), P("section", None, "tensor"), P("section", None))

    return jax.shard_map(
        on_device,
        mesh=mesh,
        in_specs=placed,
        out_specs=(P(None, AXES, None), P(None, "section", None)),
        check_vma=False,
    )
```

```python
import functools

import jax
import jax.numpy as jnp
from jax import lax
from jax.experimental import pallas as pl
from jax.experimental.pallas import tpu as pltpu
from jax.sharding import PartitionSpec as P


BLOCK = 128
AXES = ("section", "tensor")

scale_floor = 0.00390625


def partner(index, step, count):
    if count & (count - 1) == 0:
        return index ^ step
    return (index + step) % count


def origin(index, step, count):
    if count & (count - 1) == 0:
        return index ^ step
    return (index + count - step) % count


def column_gain(gain):
    return jnp.broadcast_to(gain, (BLOCK, BLOCK)).T


def fold(weight, gain):
    return (weight.astype(jnp.float32) * gain).astype(jnp.bfloat16).astype(jnp.float32)


def block_max(folded):
    largest = jnp.max(jnp.max(jnp.abs(folded), axis=0, keepdims=True), axis=1, keepdims=True)
    return jnp.maximum(largest, scale_floor)


def pack_kernel(
    steps, sections_count, ranks_count, shares, key_ref, value_ref, gain_ref, out_ref, raw, gain, sems
):
    section = lax.axis_index("section")
    rank = lax.axis_index("tensor")
    rows, head_cols = raw.shape[1:]
    to_section = partner(section, steps[0], sections_count)
    to_unit = partner(rank // shares, steps[1], ranks_count // shares)
    first = pl.multiple_of((to_section * (ranks_count // shares) + to_unit) * rows, rows)
    copies = [
        pltpu.make_async_copy(key_ref.at[0, pl.ds(first, rows)], raw.at[0], sems.at[0]),
        pltpu.make_async_copy(value_ref.at[0, pl.ds(first, rows)], raw.at[1], sems.at[1]),
        pltpu.make_async_copy(gain_ref.at[:, pl.ds(first, rows)], gain, sems.at[2]),
    ]
    for copy in copies:
        copy.start()
    for copy in reversed(copies):
        copy.wait()
    share_rows = rows // shares
    for row in range(0, rows, BLOCK):
        gains = column_gain(gain[:, row : row + BLOCK].astype(jnp.float32))
        for kind in range(2):
            for col in range(0, head_cols, BLOCK):
                folded = fold(raw[kind, row : row + BLOCK, col : col + BLOCK], gains)
                scaled = (folded / block_max(folded)).astype(jnp.bfloat16)
                to = kind * head_cols + col
                if shares == 1:
                    out_ref[0, row : row + BLOCK, to : to + BLOCK] = scaled
                    continue
                for part in range(BLOCK // share_rows):
                    place = origin(row // share_rows + part, rank % shares, shares)
                    out_ref[place, :, to : to + BLOCK] = scaled[
                        part * share_rows : (part + 1) * share_rows
                    ]


def pack(steps, sections_count, ranks_count, weights, space):
    key_weight, value_weight, norm_gain = weights
    model_rows, head_cols = key_weight.shape[1:]
    row_share = model_rows // (sections_count * ranks_count)
    shares = max(1, BLOCK // row_share)
    rows = row_share * shares
    any_ref = pl.BlockSpec(memory_space=pl.ANY)
    return pl.pallas_call(
        functools.partial(pack_kernel, steps, sections_count, ranks_count, shares),
        out_shape=space((shares, row_share, 2 * head_cols), jnp.bfloat16),
        in_specs=[any_ref] * 3,
        out_specs=pl.BlockSpec(memory_space=pltpu.VMEM),
        scratch_shapes=[
            pltpu.VMEM((2, rows, head_cols), jnp.bfloat16),
            pltpu.VMEM((1, rows), jnp.bfloat16),
            pltpu.SemaphoreType.DMA((3,)),
        ],
        compiler_params=pltpu.CompilerParams(vmem_limit_bytes=16 * 2**20),
        cost_estimate=pl.CostEstimate(
            flops=rows * head_cols * 40, bytes_accessed=rows * head_cols * 8, transcendentals=0
        ),
        name="pack",
    )(key_weight, value_weight, norm_gain)


def place_kernel(steps, sections_count, ranks_count, has_out, *refs):
    blocks = refs[: len(steps)]
    out_ref, sems = refs[len(steps) + has_out :]
    section = lax.axis_index("section")
    rank = lax.axis_index("tensor")
    head_cols = blocks[0].shape[1] // 2
    copies = []
    for index, (far, near) in enumerate(steps):
        layer = origin(section, far, sections_count)
        head = origin(rank, near, ranks_count)
        for kind in range(2):
            first = pl.multiple_of((kind * ranks_count + head) * head_cols, head_cols)
            copies.append(
                pltpu.make_async_copy(
                    blocks[index].at[:, pl.ds(kind * head_cols, head_cols)],
                    out_ref.at[layer, :, pl.ds(first, head_cols)],
                    sems.at[2 * index + kind],
                )
            )
    for copy in copies:
        copy.start()
    for copy in copies:
        copy.wait()


def place(steps, sections_count, ranks_count, blocks, out, space):
    rows, cols = blocks[0].shape
    shape = jax.ShapeDtypeStruct((sections_count, rows, ranks_count * cols), jnp.bfloat16)
    has_out = 0 if out is None else 1
    any_ref = pl.BlockSpec(memory_space=pl.ANY)
    return pl.pallas_call(
        functools.partial(place_kernel, steps, sections_count, ranks_count, has_out),
        out_shape=shape,
        in_specs=[pl.BlockSpec(memory_space=pltpu.VMEM)] * len(blocks) + [any_ref] * has_out,
        out_specs=any_ref,
        scratch_shapes=[pltpu.SemaphoreType.DMA((2 * len(steps),))],
        input_output_aliases={len(blocks): 0} if has_out else {},
        compiler_params=pltpu.CompilerParams(vmem_limit_bytes=4 * 2**20),
        cost_estimate=pl.CostEstimate(
            flops=len(steps) * rows * cols, bytes_accessed=len(steps) * rows * cols * 4, transcendentals=0
        ),
        name="place",
    )(
        *[pltpu.with_memory_space_constraint(block, space) for block in blocks],
        *([] if out is None else [out]),
    )


def scales_kernel(key_ref, value_ref, gain_ref, out_ref):
    rows, head_cols = key_ref.shape[1:]
    ranks_count = out_ref.shape[1]
    rank = lax.axis_index("tensor")
    cols_here = head_cols // BLOCK
    shape = (rows // BLOCK, BLOCK)
    row_of = lax.broadcasted_iota(jnp.int32, shape, 0)
    lane_of = lax.broadcasted_iota(jnp.int32, shape, 1)
    found = jnp.zeros(shape, jnp.float32)
    for row in range(rows // BLOCK):
        span = slice(row * BLOCK, (row + 1) * BLOCK)
        gains = column_gain(gain_ref[:, span].astype(jnp.float32))
        for kind, ref in enumerate((key_ref, value_ref)):
            for col in range(cols_here):
                folded = fold(ref[0, span, col * BLOCK : (col + 1) * BLOCK], gains)
                lane = (kind * ranks_count + rank) * cols_here + col
                here = jnp.logical_and(row_of == row, lane_of == lane)
                found = jnp.where(here, block_max(folded), found)
    for copy in range(ranks_count):
        out_ref[0, copy] = found.astype(jnp.bfloat16)


def scales(sections_count, ranks_count, weights):
    key_weight, value_weight, norm_gain = weights
    model_rows, head_cols = key_weight.shape[1:]
    rows = model_rows // sections_count
    weight_spec = pl.BlockSpec((1, rows, head_cols), lambda i: (0, i, 0))
    return pl.pallas_call(
        scales_kernel,
        grid=(sections_count,),
        out_shape=jax.ShapeDtypeStruct(
            (sections_count, ranks_count, rows // BLOCK, BLOCK), jnp.bfloat16
        ),
        in_specs=[weight_spec, weight_spec, pl.BlockSpec((1, rows), lambda i: (0, i))],
        out_specs=pl.BlockSpec((1, ranks_count, rows // BLOCK, BLOCK), lambda i: (i, 0, 0, 0)),
        compiler_params=pltpu.CompilerParams(vmem_limit_bytes=16 * 2**20),
        cost_estimate=pl.CostEstimate(
            flops=model_rows * head_cols * 20, bytes_accessed=model_rows * head_cols * 4, transcendentals=0
        ),
        name="scales",
    )(key_weight, value_weight, norm_gain)


def send_order(sections_count, units_count):
    sections = list(range(sections_count))
    if sections_count % 4 == 0:
        sections = [x for step in range(sections_count // 2) for x in (step, step ^ 3 * sections_count // 4)]
    half = units_count // 2
    early = sections_count - sections_count // 4
    crossing = [(far, unit) for far in sections[:early] for unit in reversed(range(half, units_count))]
    crossing += [(far, unit) for far in sections[early:] for unit in range(half, units_count)]
    others = [(far, unit) for far in sections for unit in reversed(range(half))]
    others.remove((0, 0))
    order = crossing[:2]
    placed = 0
    for index, step in enumerate(crossing[2:], 1):
        until = -(-len(others) * index // (len(crossing) - 2))
        order += others[placed:until] + [step]
        placed = until
    return order + [(0, 0)]


def on_device(key_weight, value_weight, norm_gain):
    sections_count = lax.axis_size("section")
    ranks_count = lax.axis_size("tensor")
    sizes = (sections_count, ranks_count)
    weights = [
        pltpu.with_memory_space_constraint(weight, pltpu.HBM)
        for weight in (key_weight, value_weight, norm_gain)
    ]
    model_rows, head_cols = key_weight.shape[1:]
    row_share = model_rows // (sections_count * ranks_count)
    shares = max(1, BLOCK // row_share)
    order = send_order(sections_count, ranks_count // shares)
    arrived = {}
    for count, (far, unit) in enumerate(order):
        space = pltpu.VMEM if count < 4 else pltpu.HBM
        packed = pack((far, unit), *sizes, weights, space)
        for part in range(shares):
            near = unit * shares + part
            pairs = [
                (
                    section * ranks_count + rank,
                    partner(section, far, sections_count) * ranks_count
                    + partner(rank, near, ranks_count),
                )
                for section in range(sections_count)
                for rank in range(ranks_count)
            ]
            block = packed[part]
            if (far, near) != (0, 0):
                block = lax.ppermute(block, AXES, pairs)
            arrived[far, near] = block
    sent_scales = scales(*sizes, weights)
    got = lax.all_to_all(
        sent_scales.reshape((sections_count * ranks_count,) + sent_scales.shape[2:]), AXES, 0, 0, tiled=True
    )
    col_blocks = 2 * ranks_count * head_cols // BLOCK
    block_scale = jnp.max(got.reshape(sent_scales.shape), axis=1)[:, :, :col_blocks].astype(jnp.float32)
    last = tuple(unit * shares + shares - 1 if i else unit for i, unit in enumerate(order[-2]))
    out = None
    groups = [[(far, near) for near in range(ranks_count) if (far, near) != last] for far in dict(order)]
    for steps in groups + [[last]]:
        space = pltpu.VMEM if len(steps) == 1 or last[0] in steps[0] else pltpu.HBM
        out = place(steps, *sizes, [arrived[step] for step in steps], out, space)
    return (out, block_scale)


def solution(mesh):
    placed = (P("section", None, "tensor"), P("section", None, "tensor"), P("section", None))

    return jax.shard_map(
        on_device,
        mesh=mesh,
        in_specs=placed,
        out_specs=(P(None, AXES, None), P(None, "section", None)),
        check_vma=False,
    )
```
